32 devices in a mesh: blk: 8 (over y, x, core), grp: 4 (over z).
Axes of the slice: x: 2, y: 2, z: 4, core: 2. Of those that a mesh axis runs over, the one named last changes fastest.
Arguments:
- samples: float32 [32, 128, 256], P('blk', 'grp'), may hold values from -11 to 11
- pair_table: int32 [32, 16], P('blk'), may hold values from 0 to 31
- assignment: int32 [2, 32], P(None, 'blk'), may hold values from 0 to 127
- band_index: int32 [2], replicated, may hold values from 0 to 1023
Outputs:
- log_weight: float32 [2, 32, 128], P(None, 'blk', 'grp')
The draws below stay inside these ranges and needn't reach their ends.
All inputs are finite; a program needn't handle non-finite values.
Results may differ from the reference program's by a relative error of at most 0.0003.
Values sent between devices are 32-bit elements; how exact they have to be, the bound alone decides.
No kernel may reach another device: no remote copies, remote signals or barrier semaphores. Data moves between devices by JAX's collectives and lax.ppermute only.
A program may use at most 128 MiB of HBM per device.

```python
import math
import jax
import jax.numpy as jnp
import numpy as np
from jax import lax

D = 256
ITERS = 2
PAIRS = 16
M = 32
S = 128


def draw_samples(key, part):
    keys_all = jax.random.split(jax.random.fold_in(key, 11), 7)
    noise = jnp.clip(jax.random.normal(keys_all[0], (M, S, D), jnp.float32), -4.0, 4.0)
    chosen = jax.random.randint(keys_all[4], (), 0, M)
    picked = (jax.random.uniform(keys_all[5], (M,), jnp.float32) < 0.25) | (jnp.arange(M) == chosen)
    sign = jnp.where(jax.random.uniform(keys_all[6], (M,), jnp.float32) < 0.5, -1.0, 1.0)
    shift = jnp.where(picked, 6.5 * sign, 0.0)[:, None, None]
    offsets = jax.random.uniform(keys_all[1], (M, 1, D), jnp.float32, -0.5, 0.5)
    return jnp.clip(offsets + noise + shift, -11.0, 11.0)


def set_ends(drawn, key, smallest, largest):
    dims = drawn.shape
    place = [jax.random.randint(jax.random.fold_in(key, axis), (), 0, dims[axis]) for axis in range(len(dims))]
    drawn = drawn.at[tuple(place)].set(smallest)
    longest = dims.index(max(dims))
    place[longest] = (place[longest] + 1) % dims[longest]
    return drawn.at[tuple(place)].set(largest)


def rank_table(amount, slope):
    loads = [(1 << 20) // math.isqrt(rank ** slope) + 1 for rank in range(1, amount + 1)]
    deviation = 1 + sum(loads) // (1 << 30)
    return np.cumsum(np.array([max(1, weight // deviation) for weight in loads]))


def ranked(own_key, dims, amount, slope):
    grid = rank_table(amount, slope)
    ticket = jax.random.randint(jax.random.fold_in(own_key, 1), dims, 0, int(grid[amount - 1]))
    grade = jnp.searchsorted(jnp.asarray(grid, jnp.int32), ticket, side="right")
    return jax.random.permutation(jax.random.fold_in(own_key, 2), amount)[grade].astype(jnp.int32)


def setup_inputs(seed: int = 0) -> dict:
    keys = jax.random.split(jax.random.key(seed), 5)
    samples = draw_samples(jax.random.fold_in(keys[4], 71), 0)
    pair_table = set_ends(ranked(keys[1], (M, PAIRS), M, 2), jax.random.fold_in(keys[1], 3), 0, M - 1).astype(jnp.int32)
    assignment = set_ends(jax.random.randint(keys[2], (ITERS, M), 0, S), jax.random.fold_in(keys[2], 1), 0, S - 1).astype(jnp.int32)
    band_index = jax.random.randint(keys[3], (ITERS,), 0, 1024).astype(jnp.int32)
    return {"samples": samples, "pair_table": pair_table, "assignment": assignment, "band_index": band_index}


def reference(samples, pair_table, assignment, band_index):
    band_sq = D * (1.0 + band_index.astype(jnp.float32) / 256.0) / 32.0
    flat = samples.reshape(M * S, D)
    flat_norm = jnp.sum(flat * flat, -1)
    members = jnp.arange(M, dtype=jnp.int32)
    picked = samples[members[None, :], assignment]
    centre = jnp.sum(picked, axis=1) / M
    counts = jnp.sum((pair_table[:, :, None] == members[None, None, :]).astype(jnp.float32), axis=1)

    def per_member(member):
        query = lax.dynamic_index_in_dim(samples, member, 0, keepdims=False)
        query_norm = jnp.sum(query * query, -1)
        product = jnp.einsum("qd,kd->qk", query, flat, precision=lax.Precision.HIGHEST)
        distance = query_norm[:, None] + flat_norm[None, :] - 2.0 * product
        stacked = []
        for turn in range(ITERS):
            scores = (-distance / (2.0 * band_sq[turn])).reshape(S, M, S)
            peak = jnp.max(scores, -1)
            stacked.append(peak + jnp.log(jnp.sum(jnp.exp(scores - peak[..., None]), -1)))
        return jnp.stack(stacked)

    kernel = lax.map(per_member, members)
    weighted = jnp.einsum("atsm,am->tas", kernel, counts, precision=lax.Precision.HIGHEST) / PAIRS
    spread = samples[None] - centre[:, None, None, :]
    logits = weighted - jnp.sum(spread * spread, -1) / (2.0 * band_sq[:, None, None])
    peak = jnp.max(logits, -1, keepdims=True)
    totals = jnp.sum(jnp.exp(logits - peak), -1, keepdims=True)
    return logits - peak - jnp.log(totals)
```

```python
import functools

import jax
import jax.numpy as jnp
from jax import lax
from jax.experimental import pallas as pl
from jax.experimental.pallas import tpu as pltpu
from jax.sharding import PartitionSpec as P

HIGH = lax.Precision.HIGHEST
NT = (((1,), (1,)), ((), ()))
NN = (((1,), (0,)), ((), ()))


def dot(a, b, dims):
    return lax.dot_general(a, b, dims, precision=HIGH, preferred_element_type=jnp.float32)


def inverse_width(band_ref, turn, width, shape):
    index = jnp.full(shape, band_ref[turn], jnp.int32).astype(jnp.float32)
    band_sq = width * (1.0 + index / 256.0) / 32.0
    return 1.0 / (2.0 * band_sq)


def prepare_kernel(group_ref, assign_ref, x_ref, out_ref, *, subs, rows, rounds):
    first = group_ref[0] * rows
    lane = lax.broadcasted_iota(jnp.int32, (8, subs * rows), 1)
    line = lax.broadcasted_iota(jnp.int32, (8, subs * rows), 0)
    weight = jnp.zeros((8, subs * rows), jnp.float32)
    for turn in range(rounds):
        for sub in range(subs):
            local = assign_ref[turn, sub] - first
            inside = jnp.logical_and(local >= 0, local < rows)
            target = jnp.where(inside, sub * rows + local, -1)
            weight = jnp.where(
                jnp.logical_and(line == turn, lane == target), 1.0, weight
            )
    x = x_ref[...]
    out_ref[: subs * rows, :] = x
    out_ref[subs * rows :, :] = dot(weight, x, NN)


def score_kernel(
    band_ref, hot_ref, *refs, blocks, groups, subs, rows, rounds, pairs, members
):
    key_refs = refs[:blocks]
    query_refs = refs[blocks : blocks + groups - 1]
    out_ref, norm_ref, queries, low, totals = refs[blocks + groups - 1 :]
    lanes = subs * rows
    width = queries.shape[1]
    count = groups * lanes
    queries[:lanes, :] = key_refs[0][:lanes, :]
    for k in range(1, groups):
        queries[k * lanes : (k + 1) * lanes, :] = query_refs[k - 1][...]
    q = queries[...]
    query_norm = dot(jnp.ones((8, width), jnp.float32), q * q, NT)[:1]
    inverse = [inverse_width(band_ref, turn, width, (1, count)) for turn in range(rounds)]
    q2 = -2.0 * q
    centre = jnp.zeros((8, width), jnp.float32)
    for block in range(blocks):
        keys = key_refs[block][:lanes, :]
        centre += key_refs[block][lanes:, :]
        key_norm = jnp.sum(keys * keys, -1, keepdims=True)
        part = (key_norm + dot(keys, q2, NT)).reshape(subs, rows, count)
        smallest = jnp.min(part, 1)
        gap = smallest[:, None, :] - part
        here = slice(block * subs, (block + 1) * subs)
        low[here, :] = smallest
        for turn in range(rounds):
            totals[turn, here, :] = jnp.sum(jnp.exp(gap * inverse[turn][:, None, :]), 1)
    centre = centre / members
    cross = dot(centre, q, NT)
    nearest = low[...] + query_norm
    hot = hot_ref[...]
    lane = lax.broadcasted_iota(jnp.int32, (pairs, lanes), 1) // rows
    for turn in range(rounds):
        value = jnp.log(totals[turn]) - nearest * inverse[turn]
        chosen = dot(hot, value, NN)
        for k in range(groups):
            piece = chosen[:, k * lanes : (k + 1) * lanes]
            merged = piece[:pairs]
            for sub in range(1, subs):
                merged = jnp.where(lane == sub, piece[sub * pairs : (sub + 1) * pairs], merged)
            at = (k * rounds + turn) * pairs
            out_ref[at : at + pairs, :] = merged
    base = groups * rounds * pairs
    for k in range(groups):
        out_ref[base + k * rounds : base + (k + 1) * rounds, :] = cross[
            :rounds, k * lanes : (k + 1) * lanes
        ]
        norm_ref[k : k + 1, :] = query_norm[:, k * lanes : (k + 1) * lanes]
    base += groups * rounds
    for c in range(width // lanes):
        out_ref[base + c * 8 : base + (c + 1) * 8, :] = centre[:, c * lanes : (c + 1) * lanes]


def finish_kernel(band_ref, norm_ref, *refs, groups, subs, rows, rounds, pairs, width):
    parts = refs[:groups]
    out_ref = refs[groups]
    lanes = subs * rows
    base = groups * rounds * pairs
    tail = base + groups * rounds
    centre = [
        sum(part[tail + c * 8 : tail + (c + 1) * 8, :] for part in parts)
        for c in range(width // lanes)
    ]
    centre_sq = sum(jnp.sum(c * c, -1, keepdims=True) for c in centre)
    group_of = lax.broadcasted_iota(jnp.int32, (1, lanes), 1) // rows
    for turn in range(rounds):
        inverse = inverse_width(band_ref, turn, width, (1, lanes))
        logits = []
        for k in range(groups):
            pieces = []
            cross = jnp.zeros((1, lanes), jnp.float32)
            for j in range(groups):
                at = ((k ^ j) * rounds + turn) * pairs
                pieces.append(parts[j][at : at + pairs, :])
                row = base + (k ^ j) * rounds + turn
                cross = cross + parts[j][row : row + 1, :]
            peak = functools.reduce(jnp.maximum, pieces)
            total = sum(jnp.exp(piece - peak) for piece in pieces)
            kernel = peak + jnp.log(total)
            weighted = jnp.sum(kernel, 0, keepdims=True) / pairs
            spread = norm_ref[k : k + 1, :] - 2.0 * cross + centre_sq[turn : turn + 1, :]
            logits.append(weighted - spread * inverse)
        peak = functools.reduce(jnp.maximum, logits)
        row_peak = jnp.zeros((1, lanes), jnp.float32)
        for sub in range(subs):
            here = jnp.max(jnp.where(group_of == sub, peak, -jnp.inf), -1, keepdims=True)
            row_peak = jnp.where(group_of == sub, here, row_peak)
        total = sum(jnp.exp(value - row_peak) for value in logits)
        for sub in range(subs):
            here = jnp.sum(jnp.where(group_of == sub, total, 0.0), -1, keepdims=True)
            value = logits[0] - row_peak - jnp.log(here)
            out_ref[turn, sub : sub + 1, :] = value[:, sub * rows : (sub + 1) * rows]


def per_device(samples, pair_table, assignment, band_index):
    subs, rows, width = samples.shape
    rounds = assignment.shape[0]
    pairs = pair_table.shape[1]
    groups = lax.axis_size("grp")
    blocks = lax.axis_size("blk")
    members = subs * blocks
    lanes = subs * rows
    group = lax.axis_index("grp")
    block = lax.axis_index("blk")

    def over(axis, size, value, k):
        return lax.ppermute(value, axis, [(i, i ^ k) for i in range(size)])

    smem = pl.BlockSpec(memory_space=pltpu.SMEM)
    vmem = pl.BlockSpec(memory_space=pltpu.VMEM)
    x = samples.reshape(lanes, width)
    queries = [over("grp", groups, x, k) for k in range(1, groups)]
    own = pl.pallas_call(
        functools.partial(prepare_kernel, subs=subs, rows=rows, rounds=rounds),
        out_shape=jax.ShapeDtypeStruct((lanes + 8, width), jnp.float32),
        in_specs=[smem, smem, vmem],
        out_specs=vmem,
        name="prepare",
    )(group[None], assignment, x)
    keys = {0: own}
    for k in range(2, blocks, 2):
        keys[k] = over("blk", blocks, own, k)
    for k in range(0, blocks, 2):
        keys[k ^ 1] = over("blk", blocks, keys[k], 1)
    place = (pair_table // subs ^ block) * subs + pair_table % subs
    hot = (
        place.reshape(subs * pairs, 1) == jnp.arange(members, dtype=jnp.int32)[None, :]
    ).astype(jnp.float32)
    height = groups * rounds * pairs + groups * rounds + 8 * (width // lanes)
    part, norm = pl.pallas_call(
        functools.partial(
            score_kernel,
            blocks=blocks,
            groups=groups,
            subs=subs,
            rows=rows,
            rounds=rounds,
            pairs=pairs,
            members=members,
        ),
        out_shape=(
            jax.ShapeDtypeStruct((height, lanes), jnp.float32),
            jax.ShapeDtypeStruct((groups, lanes), jnp.float32),
        ),
        in_specs=[smem] + [vmem] * (blocks + groups),
        out_specs=(vmem, vmem),
        scratch_shapes=[
            pltpu.VMEM((groups * lanes, width), jnp.float32),
            pltpu.VMEM((members, groups * lanes), jnp.float32),
            pltpu.VMEM((rounds, members, groups * lanes), jnp.float32),
        ],
        name="score",
    )(band_index, hot, *[keys[k] for k in range(blocks)], *queries)
    parts = [part] + [over("grp", groups, part, k) for k in range(1, groups)]
    return pl.pallas_call(
        functools.partial(
            finish_kernel,
            groups=groups,
            subs=subs,
            rows=rows,
            rounds=rounds,
            pairs=pairs,
            width=width,
        ),
        out_shape=jax.ShapeDtypeStruct((rounds, subs, rows), jnp.float32),
        in_specs=[smem] + [vmem] * (groups + 1),
        out_specs=vmem,
        name="finish",
    )(band_index, norm, *parts)


def solution(mesh):
    return jax.shard_map(
        per_device,
        mesh=mesh,
        in_specs=(P("blk", "grp", None), P("blk", None), P(None, "blk"), P()),
        out_specs=P(None, "blk", "grp"),
        check_vma=False,
    )
```

```python
import functools

import jax
import jax.numpy as jnp
from jax import lax
from jax.experimental import pallas as pl
from jax.experimental.pallas import tpu as pltpu
from jax.sharding import PartitionSpec as P


GRANT = pltpu.CompilerParams(vmem_limit_bytes=16 * 2**20)
HIGH = lax.Precision.HIGHEST
NN = (((1,), (0,)), ((), ()))
LEFT = (0, 0, 1, 1, 0, 2)
RIGHT = (0, 1, 0, 1, 2, 0)


def split(value):
    first = value.astype(jnp.bfloat16)
    rest = value - first.astype(jnp.float32)
    second = rest.astype(jnp.bfloat16)
    third = (rest - second.astype(jnp.float32)).astype(jnp.bfloat16)
    return first, second, third


def product(left, right):
    a = split(left)
    return lax.dot_general(
        jnp.concatenate([a[k] for k in LEFT], 1), right, NN, preferred_element_type=jnp.float32
    )


def inverse_width(band_ref, turn, width, shape):
    index = jnp.full(shape, band_ref[turn], jnp.int32).astype(jnp.float32)
    band_sq = width * (1.0 + index / 256.0) / 32.0
    return 1.0 / (2.0 * band_sq)


def prepare_kernel(group_ref, assign_ref, x_ref, out_ref, *, subs, rows, rounds):
    lanes = subs * rows
    first = group_ref[0] * rows
    lane = lax.broadcasted_iota(jnp.int32, (8, lanes), 1)
    line = lax.broadcasted_iota(jnp.int32, (8, lanes), 0)
    weight = jnp.zeros((8, lanes), jnp.float32)
    for turn in range(rounds):
        for sub in range(subs):
            local = assign_ref[turn, sub] - first
            inside = jnp.logical_and(local >= 0, local < rows)
            target = jnp.where(inside, sub * rows + local, -1)
            weight = jnp.where(
                jnp.logical_and(line == turn, lane == target), 1.0, weight
            )
    x = x_ref[...]
    out_ref[:lanes, :] = x
    out_ref[lanes:, :] = lax.dot_general(
        weight, x, NN, precision=HIGH, preferred_element_type=jnp.float32
    )


def layout(groups, rounds, pairs, width, lanes):
    cross = groups * rounds * pairs
    norm = cross + groups * rounds
    centre = norm + groups
    height = centre + rounds * (width // lanes)
    return cross, norm, centre, -(-height // 8) * 8


def score_kernel(
    band_ref, hot_ref, *refs, chunks, blocks, groups, subs, rows, rounds, pairs, members, fresh
):
    key_refs = refs[:blocks]
    query_refs = refs[blocks : blocks + len(chunks)]
    rest = refs[blocks + len(chunks) :]
    out_ref, terms, low, totals = rest if fresh else rest[1:]
    if not fresh:
        out_ref[...] = rest[0][...]
    lanes = subs * rows
    width = key_refs[0].shape[1]
    count = len(chunks) * lanes
    cross_at, norm_at, centre_at, _ = layout(groups, rounds, pairs, width, lanes)
    q = jnp.concatenate([ref[:lanes, :].T for ref in query_refs], 1)
    query_norm = jnp.sum(q * q, 0, keepdims=True)
    b = split(-2.0 * q)
    for at, k in enumerate(RIGHT):
        terms[at * width : (at + 1) * width, :] = b[k]
    right = terms[...]
    inverse = [inverse_width(band_ref, turn, width, (1, count)) for turn in range(rounds)]
    centre = jnp.zeros((8, width), jnp.float32)
    for block in range(blocks):
        keys = key_refs[block][:lanes, :]
        centre += key_refs[block][lanes:, :]
        key_norm = jnp.sum(keys * keys, -1, keepdims=True)
        part = (key_norm + product(keys, right)).reshape(subs, rows, count)
        smallest = jnp.min(part, 1)
        gap = smallest[:, None, :] - part
        here = slice(block * subs, (block + 1) * subs)
        low[here, :] = smallest
        for turn in range(rounds):
            totals[turn, here, :] = jnp.sum(jnp.exp(gap * inverse[turn][:, None, :]), 1)
    centre = centre / members
    cross = product(centre, right)
    nearest = low[...] + query_norm
    hot = hot_ref[...]
    lane = lax.broadcasted_iota(jnp.int32, (pairs, lanes), 1) // rows
    for turn in range(rounds):
        value = jnp.log(totals[turn]) - nearest * inverse[turn]
        chosen = lax.dot_general(
            hot, value, NN, precision=HIGH, preferred_element_type=jnp.float32
        )
        for i, k in enumerate(chunks):
            piece = chosen[:, i * lanes : (i + 1) * lanes]
            merged = piece[:pairs]
            for sub in range(1, subs):
                merged = jnp.where(lane == sub, piece[sub * pairs : (sub + 1) * pairs], merged)
            at = (k * rounds + turn) * pairs
            out_ref[at : at + pairs, :] = merged
    for i, k in enumerate(chunks):
        out_ref[cross_at + k * rounds : cross_at + (k + 1) * rounds, :] = cross[
            :rounds, i * lanes : (i + 1) * lanes
        ]
        out_ref[norm_at + k : norm_at + k + 1, :] = query_norm[:, i * lanes : (i + 1) * lanes]
    if fresh:
        for turn in range(rounds):
            for c in range(width // lanes):
                at = centre_at + turn * (width // lanes) + c
                out_ref[at : at + 1, :] = centre[
                    turn : turn + 1, c * lanes : (c + 1) * lanes
                ]


def finish_kernel(band_ref, *refs, groups, subs, rows, rounds, pairs, width):
    parts = refs[:groups]
    out_ref = refs[groups]
    lanes = subs * rows
    cross_at, norm_at, centre_at, _ = layout(groups, rounds, pairs, width, lanes)
    step = rounds * pairs
    sums = []
    cross = []
    for k in range(groups):
        pieces = [parts[j][(k ^ j) * step : ((k ^ j) + 1) * step, :] for j in range(groups)]
        peak = functools.reduce(jnp.maximum, pieces)
        total = sum(jnp.exp(piece - peak) for piece in pieces)
        sums.append(peak + jnp.log(total))
        at = [cross_at + (k ^ j) * rounds for j in range(groups)]
        cross.append(sum(parts[j][at[j] : at[j] + rounds, :] for j in range(groups)))
    kernel = jnp.concatenate(sums, 0).reshape(groups * rounds, pairs, lanes)
    weighted = jnp.sum(kernel, 1) / pairs
    cross = jnp.concatenate(cross, 0)
    halves = width // lanes
    centre = sum(part[centre_at : centre_at + rounds * halves, :] for part in parts)
    centre_sq = jnp.sum(centre * centre, -1, keepdims=True)
    group_of = lax.broadcasted_iota(jnp.int32, (1, lanes), 1) // rows
    line = lax.broadcasted_iota(jnp.int32, (groups * rounds, lanes), 0)
    inverse = inverse_width(band_ref, rounds - 1, width, (groups * rounds, lanes))
    constant = jnp.zeros((groups * rounds, lanes), jnp.float32)
    norm = jnp.zeros((groups * rounds, lanes), jnp.float32)
    for turn in range(rounds):
        mine = line % rounds == turn
        inverse = jnp.where(
            mine, inverse_width(band_ref, turn, width, (groups * rounds, lanes)), inverse
        )
        square = sum(
            centre_sq[turn * halves + c : turn * halves + c + 1, :] for c in range(halves)
        )
        constant = jnp.where(mine, square, constant)
    for k in range(groups):
        norm = jnp.where(line // rounds == k, parts[0][norm_at + k : norm_at + k + 1, :], norm)
    logits = weighted - (norm + cross + constant) * inverse

    def over_draws(value, combine, reduce, neutral):
        shift = rounds
        while shift < groups * rounds:
            value = combine(value, pltpu.roll(value, shift, 0))
            shift *= 2
        result = value
        for sub in range(subs):
            here = reduce(jnp.where(group_of == sub, value, neutral), -1, keepdims=True)
            result = jnp.where(group_of == sub, here, result)
        return result

    peak = over_draws(logits, jnp.maximum, jnp.max, -jnp.inf)
    shifted = logits - peak
    total = over_draws(jnp.exp(shifted), jnp.add, jnp.sum, 0.0)
    value = shifted - jnp.log(total)
    for turn in range(rounds):
        for sub in range(subs):
            out_ref[turn, sub : sub + 1, :] = value[
                turn : turn + 1, sub * rows : (sub + 1) * rows
            ]


def per_device(samples, pair_table, assignment, band_index):
    subs, rows, width = samples.shape
    rounds = assignment.shape[0]
    pairs = pair_table.shape[1]
    groups = lax.axis_size("grp")
    blocks = lax.axis_size("blk")
    members = subs * blocks
    lanes = subs * rows
    group = lax.axis_index("grp")
    block = lax.axis_index("blk")

    def over(axis, size, value, k):
        with jax.named_scope(f"{axis}{k}"):
            return lax.ppermute(value, axis, [(i, i ^ k) for i in range(size)])

    smem = pl.BlockSpec(memory_space=pltpu.SMEM)
    vmem = pl.BlockSpec(memory_space=pltpu.VMEM)
    x = samples.reshape(lanes, width)
    queries = {k: over("grp", groups, x, k) for k in range(groups - 1, 0, -1)}
    own = pl.pallas_call(
        functools.partial(prepare_kernel, subs=subs, rows=rows, rounds=rounds),
        out_shape=jax.ShapeDtypeStruct((lanes + 8, width), jnp.float32),
        in_specs=[smem, smem, vmem],
        out_specs=vmem,
        compiler_params=GRANT,
        name="prepare",
    )(group[None], assignment, x)
    keys = {0: own}
    for k in range(2, blocks, 2):
        keys[k] = over("blk", blocks, own, k)
    for k in range(0, blocks, 2):
        keys[k ^ 1] = over("blk", blocks, keys[k], 1)
    queries[0] = own
    place = (pair_table // subs ^ block) * subs + pair_table % subs
    hot = (
        place.reshape(subs * pairs, 1) == jnp.arange(members, dtype=jnp.int32)[None, :]
    ).astype(jnp.float32)
    height = layout(groups, rounds, pairs, width, lanes)[-1]

    def score(chunks, previous):
        fresh = previous is None
        count = len(chunks) * lanes
        return pl.pallas_call(
            functools.partial(
                score_kernel,
                chunks=chunks,
                blocks=blocks,
                groups=groups,
                subs=subs,
                rows=rows,
                rounds=rounds,
                pairs=pairs,
                members=members,
                fresh=fresh,
            ),
            out_shape=jax.ShapeDtypeStruct((height, lanes), jnp.float32),
            in_specs=[smem] + [vmem] * (1 + blocks + len(chunks) + (not fresh)),
            out_specs=vmem,
            scratch_shapes=[
                pltpu.VMEM((len(RIGHT) * width, count), jnp.bfloat16),
                pltpu.VMEM((members, count), jnp.float32),
                pltpu.VMEM((rounds, members, count), jnp.float32),
            ],
            input_output_aliases={} if fresh else {2 + blocks + len(chunks): 0},
            compiler_params=GRANT,
            name="score",
        )(
            band_index,
            hot,
            *[keys[k] for k in range(blocks)],
            *[queries[k] for k in chunks],
            *([] if fresh else [previous]),
        )

    part = None
    for first in range(0, groups, 2):
        part = score(list(range(groups))[first : first + 2], part)
    parts = {k: over("grp", groups, part, k) for k in range(groups - 1, 0, -1)}
    parts[0] = part
    return pl.pallas_call(
        functools.partial(
            finish_kernel,
            groups=groups,
            subs=subs,
            rows=rows,
            rounds=rounds,
            pairs=pairs,
            width=width,
        ),
        out_shape=jax.ShapeDtypeStruct((rounds, subs, rows), jnp.float32),
        in_specs=[smem] + [vmem] * groups,
        out_specs=vmem,
        compiler_params=GRANT,
        name="finish",
    )(band_index, *[parts[k] for k in range(groups)])


def solution(mesh):
    return jax.shard_map(
        per_device,
        mesh=mesh,
        in_specs=(P("blk", "grp", None), P("blk", None), P(None, "blk"), P()),
        out_specs=P(None, "blk", "grp"),
        check_vma=False,
    )
```

```python
import functools

import jax
import jax.numpy as jnp
from jax import lax
from jax.experimental import pallas as pl
from jax.experimental.pallas import tpu as pltpu
from jax.sharding import PartitionSpec as P


HIGH = lax.Precision.HIGHEST
NN = (((1,), (0,)), ((), ()))
LOG2E = 1.4426950408889634
LEFT = (0, 0, 1, 1, 0, 2)
RIGHT = (0, 1, 0, 1, 2, 0)


def split(value):
    first = value.astype(jnp.bfloat16)
    rest = value - first.astype(jnp.float32)
    second = rest.astype(jnp.bfloat16)
    third = (rest - second.astype(jnp.float32)).astype(jnp.bfloat16)
    return first, second, third


def fill(stack, at, value, order, axis):
    parts = split(value)
    for i, k in enumerate(order):
        size = value.shape[axis]
        if axis:
            stack[at : at + value.shape[0], i * size : (i + 1) * size] = parts[k]
        else:
            stack[i * size : (i + 1) * size, at : at + value.shape[1]] = parts[k]


def prepare_kernel(first_ref, assign_hbm, x_hbm, out_ref, assign_ref, sems, *, subs, rows, rounds):
    lanes = subs * rows
    assign = pltpu.make_async_copy(assign_hbm, assign_ref, sems.at[0])
    assign.start()
    load = pltpu.make_async_copy(x_hbm, out_ref.at[pl.ds(0, lanes)], sems.at[1])
    load.start()
    lane = lax.broadcasted_iota(jnp.int32, (8, lanes), 1)
    line = lax.broadcasted_iota(jnp.int32, (8, lanes), 0)
    own = lane % rows + first_ref[...]
    assign.wait()
    weight = jnp.zeros((8, lanes), jnp.float32)
    for turn in range(rounds):
        for sub in range(subs):
            mine = (line == turn) & (lane // rows == sub)
            chosen = assign_ref[turn : turn + 1, sub : sub + 1]
            weight = jnp.where(mine & (own == chosen), 1.0, weight)
    load.wait()
    out_ref[lanes:, :] = lax.dot_general(
        weight, out_ref[:lanes, :], NN, precision=HIGH, preferred_element_type=jnp.float32
    )


def layout(groups, rounds, pairs, width, lanes):
    cross = groups * rounds * pairs
    norm = cross + groups * rounds
    centre = norm + groups
    height = centre + rounds * (width // lanes)
    return cross, norm, centre, -(-height // 8) * 8


def wide(row, count):
    return jnp.concatenate([row] * (count // row.shape[1]), 1)


def take_queries(refs, lanes, terms, norm):
    for i, ref in enumerate(refs):
        q = ref[:lanes, :].T
        here = slice(i * lanes, (i + 1) * lanes)
        norm[:, here] = jnp.broadcast_to(jnp.sum(q * q, 0, keepdims=True), (8, lanes))
        fill(terms, i * lanes, -2.0 * q, RIGHT, 0)


def take_keys(refs, lanes, stack):
    for i, ref in enumerate(refs):
        fill(stack, i * lanes, ref[:lanes, :], LEFT, 1)


def scan(
    inverse_ref, refs, stack, terms, low, totals, *, first, columns, subs, rows, rounds
):
    lanes = subs * rows
    count = terms.shape[1]
    part = lax.dot_general(stack[...], terms[...], NN, preferred_element_type=jnp.float32)
    inverse = [wide(LOG2E * inverse_ref[t : t + 1, :], count) for t in range(rounds)]
    for i, ref in enumerate(refs):
        keys = ref[:lanes, :]
        norm = jnp.sum(keys * keys, -1, keepdims=True)
        for sub in range(subs):
            mine = slice(sub * rows, (sub + 1) * rows)
            tile = part[i * lanes + sub * rows : i * lanes + (sub + 1) * rows] + norm[mine]
            smallest = jnp.min(tile, 0, keepdims=True)
            gap = smallest - tile
            at = (first + i) * subs + sub
            low[at : at + 1, columns] = smallest
            for turn in range(rounds):
                totals[turn, at : at + 1, columns] = jnp.sum(
                    jnp.exp2(gap * inverse[turn]), 0, keepdims=True
                )


def early_kernel(inverse_ref, *refs, near, chunks, subs, rows, rounds):
    lanes = subs * rows
    key_refs = refs[:near]
    query_refs = refs[near : near + chunks]
    terms, norm, stack, low, totals = refs[near + chunks :]
    take_queries(query_refs, lanes, terms, norm)
    take_keys(key_refs, lanes, stack)
    scan(
        inverse_ref,
        key_refs,
        stack,
        terms,
        low,
        totals,
        first=0,
        columns=slice(None),
        subs=subs,
        rows=rows,
        rounds=rounds,
    )


def score_kernel(
    inverse_ref,
    hot_ref,
    near_terms,
    near_norm,
    near_stack,
    near_low,
    near_totals,
    *refs,
    chunks,
    later,
    near,
    blocks,
    groups,
    subs,
    rows,
    rounds,
    pairs,
    members,
):
    key_refs = refs[:blocks]
    query_refs = refs[blocks : blocks + len(later)]
    out_ref, terms, norm, stack, low, totals = refs[blocks + len(later) :]
    lanes = subs * rows
    width = key_refs[0].shape[1]
    before = len(chunks) * lanes
    count = before + len(later) * lanes
    cross_at, norm_at, centre_at, _ = layout(groups, rounds, pairs, width, lanes)
    sizes = {"subs": subs, "rows": rows, "rounds": rounds}
    old, new = slice(0, before), slice(before, count)
    take_keys(key_refs[near:], lanes, stack)
    scan(
        inverse_ref, key_refs[near:], stack, near_terms, low, totals, first=near, columns=old, **sizes
    )
    take_queries(query_refs, lanes, terms, norm)
    scan(
        inverse_ref, key_refs[:near], near_stack, terms, low, totals, first=0, columns=new, **sizes
    )
    scan(
        inverse_ref, key_refs[near:], stack, terms, low, totals, first=near, columns=new, **sizes
    )
    done = near * subs
    low[:done, old] = near_low[...]
    totals[:, :done, old] = near_totals[...]
    centre = sum(ref[lanes:, :] for ref in key_refs) / members
    a = split(centre)
    left = jnp.concatenate([a[k] for k in LEFT], 1)
    cross = jnp.concatenate(
        [
            lax.dot_general(left, right[...], NN, preferred_element_type=jnp.float32)
            for right in (near_terms, terms)
        ],
        1,
    )
    query_norm = jnp.concatenate([near_norm[:1, :], norm[:1, :]], 1)
    nearest = low[...] + query_norm
    hot = hot_ref[...]
    lane = lax.broadcasted_iota(jnp.int32, (pairs, lanes), 1) // rows
    every = tuple(chunks) + tuple(later)
    for turn in range(rounds):
        value = jnp.log(totals[turn]) - nearest * wide(inverse_ref[turn : turn + 1, :], count)
        chosen = lax.dot_general(
            hot, value, NN, precision=HIGH, preferred_element_type=jnp.float32
        )
        for i, k in enumerate(every):
            piece = chosen[:, i * lanes : (i + 1) * lanes]
            merged = piece[:pairs]
            for sub in range(1, subs):
                merged = jnp.where(lane == sub, piece[sub * pairs : (sub + 1) * pairs], merged)
            at = (k * rounds + turn) * pairs
            out_ref[at : at + pairs, :] = merged
    for i, k in enumerate(every):
        out_ref[cross_at + k * rounds : cross_at + (k + 1) * rounds, :] = cross[
            :rounds, i * lanes : (i + 1) * lanes
        ]
        out_ref[norm_at + k : norm_at + k + 1, :] = query_norm[:, i * lanes : (i + 1) * lanes]
    for turn in range(rounds):
        for c in range(width // lanes):
            at = centre_at + turn * (width // lanes) + c
            out_ref[at : at + 1, :] = centre[turn : turn + 1, c * lanes : (c + 1) * lanes]


def finish_kernel(inverse_ref, *refs, groups, subs, rows, rounds, pairs, width):
    parts = refs[:groups]
    out_ref = refs[groups]
    lanes = subs * rows
    cross_at, norm_at, centre_at, _ = layout(groups, rounds, pairs, width, lanes)
    step = rounds * pairs
    sums = []
    cross = []
    for k in range(groups):
        pieces = [parts[j][(k ^ j) * step : ((k ^ j) + 1) * step, :] for j in range(groups)]
        peak = functools.reduce(jnp.maximum, pieces)
        total = sum(jnp.exp(piece - peak) for piece in pieces)
        sums.append(peak + jnp.log(total))
        at = [cross_at + (k ^ j) * rounds for j in range(groups)]
        cross.append(sum(parts[j][at[j] : at[j] + rounds, :] for j in range(groups)))
    kernel = jnp.concatenate(sums, 0).reshape(groups * rounds, pairs, lanes)
    weighted = jnp.sum(kernel, 1) / pairs
    cross = jnp.concatenate(cross, 0)
    halves = width // lanes
    centre = sum(part[centre_at : centre_at + rounds * halves, :] for part in parts)
    centre_sq = jnp.sum(centre * centre, -1, keepdims=True)
    group_of = lax.broadcasted_iota(jnp.int32, (1, lanes), 1) // rows
    line = lax.broadcasted_iota(jnp.int32, (groups * rounds, lanes), 0)
    inverse = jnp.zeros((groups * rounds, lanes), jnp.float32)
    constant = jnp.zeros((groups * rounds, lanes), jnp.float32)
    norm = jnp.zeros((groups * rounds, lanes), jnp.float32)
    for turn in range(rounds):
        mine = line % rounds == turn
        inverse = jnp.where(mine, inverse_ref[turn : turn + 1, :], inverse)
        square = sum(
            centre_sq[turn * halves + c : turn * halves + c + 1, :] for c in range(halves)
        )
        constant = jnp.where(mine, square, constant)
    for k in range(groups):
        norm = jnp.where(line // rounds == k, parts[0][norm_at + k : norm_at + k + 1, :], norm)
    logits = weighted - (norm + cross + constant) * inverse

    def over_draws(value, combine, reduce, neutral):
        shift = rounds
        while shift < groups * rounds:
            value = combine(value, pltpu.roll(value, shift, 0))
            shift *= 2
        result = value
        for sub in range(subs):
            here = reduce(jnp.where(group_of == sub, value, neutral), -1, keepdims=True)
            result = jnp.where(group_of == sub, here, result)
        return result

    peak = over_draws(logits, jnp.maximum, jnp.max, -jnp.inf)
    shifted = logits - peak
    total = over_draws(jnp.exp(shifted), jnp.add, jnp.sum, 0.0)
    value = shifted - jnp.log(total)
    for turn in range(rounds):
        for sub in range(subs):
            out_ref[turn, sub : sub + 1, :] = value[
                turn : turn + 1, sub * rows : (sub + 1) * rows
            ]


def program(samples, pair_table, assignment, band_index):
    subs, rows, width = samples.shape
    rounds = assignment.shape[0]
    pairs = pair_table.shape[1]
    groups = lax.axis_size("grp")
    blocks = lax.axis_size("blk")
    members = subs * blocks
    lanes = subs * rows
    group = lax.axis_index("grp")
    block = lax.axis_index("blk")

    def over(axis, size, value, k):
        return lax.ppermute(value, axis, [(i, i ^ k) for i in range(size)])

    vmem = pl.BlockSpec(memory_space=pltpu.VMEM)
    hbm = pl.BlockSpec(memory_space=pl.ANY)

    def call(kernel, shapes, arrays, scratch=(), **sizes):
        one = not isinstance(shapes, list)
        outs = [
            jax.ShapeDtypeStruct(shape[:-1], shape[-1])
            for shape in ([shapes] if one else shapes)
        ]
        return pl.pallas_call(
            functools.partial(kernel, **sizes),
            out_shape=outs[0] if one else outs,
            in_specs=[vmem] * len(arrays),
            out_specs=vmem if one else [vmem] * len(outs),
            scratch_shapes=[pltpu.VMEM(shape[:-1], shape[-1]) for shape in scratch],
            compiler_params=pltpu.CompilerParams(
                vmem_limit_bytes=(16 if blocks <= 8 else 48) * 2**20
            ),
        )(*arrays)

    f32, bf16 = jnp.float32, jnp.bfloat16
    x = samples.reshape(lanes, width)
    queries = {k: over("grp", groups, x, k) for k in range(groups - 1, 0, -1)}
    own = pl.pallas_call(
        functools.partial(prepare_kernel, subs=subs, rows=rows, rounds=rounds),
        out_shape=jax.ShapeDtypeStruct((lanes + 8, width), f32),
        in_specs=[vmem, hbm, hbm],
        out_specs=vmem,
        scratch_shapes=[
            pltpu.VMEM((rounds, subs), jnp.int32),
            pltpu.SemaphoreType.DMA((2,)),
        ],
        compiler_params=pltpu.CompilerParams(vmem_limit_bytes=4 * 2**20),
        name="prepare",
    )(jnp.full((1, lanes), group * rows, jnp.int32), assignment, x)
    keys = {0: own}
    for k in range(2, blocks, 2):
        keys[k] = over("blk", blocks, own, k)
    for k in range(0, blocks, 2):
        keys[k ^ 1] = over("blk", blocks, keys[k], 1)
    queries[0] = own
    place = (pair_table // subs ^ block) * subs + pair_table % subs
    hot = (
        place.reshape(subs * pairs, 1) == jnp.arange(members, dtype=jnp.int32)[None, :]
    ).astype(f32)
    band_sq = width * (1.0 + band_index.astype(f32) / 256.0) / 32.0
    inverse = jnp.broadcast_to((1.0 / (2.0 * band_sq))[:, None], (rounds, lanes))
    height = layout(groups, rounds, pairs, width, lanes)[-1]
    order = CHUNKS if groups == len(CHUNKS) else tuple(range(groups))
    chunks, later = order[: groups // 2], order[groups // 2 :]
    near = blocks // 2
    before, after = len(chunks) * lanes, len(later) * lanes
    sizes = {"subs": subs, "rows": rows, "rounds": rounds}
    known = call(
        early_kernel,
        [
            (len(RIGHT) * width, before, bf16),
            (8, before, f32),
            (near * lanes, len(LEFT) * width, bf16),
            (near * subs, before, f32),
            (rounds, near * subs, before, f32),
        ],
        [inverse] + [keys[k] for k in range(near)] + [queries[k] for k in chunks],
        near=near,
        chunks=len(chunks),
        **sizes,
    )
    part = call(
        score_kernel,
        (height, lanes, f32),
        [inverse, hot, *known]
        + [keys[k] for k in range(blocks)]
        + [queries[k] for k in later],
        scratch=[
            (len(RIGHT) * width, after, bf16),
            (8, after, f32),
            ((blocks - near) * lanes, len(LEFT) * width, bf16),
            (members, before + after, f32),
            (rounds, members, before + after, f32),
        ],
        chunks=chunks,
        later=later,
        near=near,
        blocks=blocks,
        groups=groups,
        pairs=pairs,
        members=members,
        **sizes,
    )
    parts = {k: over("grp", groups, part, k) for k in range(groups - 1, 0, -1)}
    parts[0] = part
    return call(
        finish_kernel,
        (rounds, subs, rows, f32),
        [inverse] + [parts[k] for k in range(groups)],
        groups=groups,
        pairs=pairs,
        width=width,
        **sizes,
    )


CHUNKS = (0, 2, 3, 1)


def solution(mesh):
    return jax.shard_map(
        program,
        mesh=mesh,
        in_specs=(P("blk", "grp", None), P("blk", None), P(None, "blk"), P()),
        out_specs=P(None, "blk", "grp"),
        check_vma=False,
    )
```

```python
import functools

import jax
import jax.numpy as jnp
from jax import lax
from jax.experimental import pallas as pl
from jax.experimental.pallas import tpu as pltpu
from jax.sharding import PartitionSpec as P


HIGH = lax.Precision.HIGHEST
NN = (((1,), (0,)), ((), ()))
LOG2E = 1.4426950408889634
LEFT = (0, 0, 1, 1, 0, 2)
RIGHT = (0, 1, 0, 1, 2, 0)


def split(value):
    first = value.astype(jnp.bfloat16)
    rest = value - first.astype(jnp.float32)
    second = rest.astype(jnp.bfloat16)
    third = (rest - second.astype(jnp.float32)).astype(jnp.bfloat16)
    return first, second, third


def fill(stack, at, value, order, axis):
    parts = split(value)
    for i, k in enumerate(order):
        size = value.shape[axis]
        if axis:
            stack[at : at + value.shape[0], i * size : (i + 1) * size] = parts[k]
        else:
            stack[i * size : (i + 1) * size, at : at + value.shape[1]] = parts[k]


def prepare_kernel(
    assign_hbm,
    table_hbm,
    band_hbm,
    x_hbm,
    out_ref,
    hot_ref,
    inverse_ref,
    assign_ref,
    table_ref,
    band_ref,
    sems,
    *,
    subs,
    rows,
    rounds,
    pairs,
):
    lanes = subs * rows
    width = out_ref.shape[1]
    copies = [
        pltpu.make_async_copy(source, target, sems.at[i])
        for i, (source, target) in enumerate(
            (
                (assign_hbm, assign_ref),
                (band_hbm, band_ref),
                (table_hbm, table_ref),
                (x_hbm, out_ref.at[pl.ds(0, lanes)]),
            )
        )
    ]
    for copy in copies:
        copy.start()
    for copy in copies[:-1]:
        copy.wait()
    block, first = lax.axis_index("blk"), lax.axis_index("grp") * rows
    lane = lax.broadcasted_iota(jnp.int32, (8, lanes), 1)
    line = lax.broadcasted_iota(jnp.int32, (8, lanes), 0)
    weight = jnp.zeros((8, lanes), jnp.float32)
    for turn in range(rounds):
        for sub in range(subs):
            local = assign_ref[turn, sub] - first
            inside = jnp.logical_and(local >= 0, local < rows)
            target = jnp.where(inside, sub * rows + local, -1)
            weight = jnp.where((line == turn) & (lane == target), 1.0, weight)
        index = jnp.full((1, lanes), band_ref[turn], jnp.int32).astype(jnp.float32)
        band_sq = width * (1.0 + index / 256.0) / 32.0
        inverse_ref[turn : turn + 1, :] = 1.0 / (2.0 * band_sq)
    members = hot_ref.shape[1]
    column = lax.broadcasted_iota(jnp.int32, (8, members), 1)
    line = lax.broadcasted_iota(jnp.int32, (8, members), 0)
    for base in range(0, subs * pairs, 8):
        target = jnp.zeros((8, members), jnp.int32)
        for i in range(8):
            entry = table_ref[(base + i) // pairs, (base + i) % pairs]
            owner = lax.div(entry, jnp.int32(subs))
            at = (owner ^ block) * subs + (entry - owner * subs)
            target = jnp.where(line == i, at, target)
        hot_ref[base : base + 8, :] = (column == target).astype(jnp.float32)
    copies[-1].wait()
    out_ref[lanes:, :] = lax.dot_general(
        weight, out_ref[:lanes, :], NN, precision=HIGH, preferred_element_type=jnp.float32
    )


def layout(groups, rounds, pairs, width, lanes):
    cross = groups * rounds * pairs
    norm = cross + groups * rounds
    centre = norm + groups
    height = centre + rounds * (width // lanes)
    return cross, norm, centre, -(-height // 8) * 8


def wide(row, count):
    return jnp.concatenate([row] * (count // row.shape[1]), 1)


def take_queries(refs, lanes, terms, norm):
    for i, ref in enumerate(refs):
        q = ref[:lanes, :].T
        here = slice(i * lanes, (i + 1) * lanes)
        norm[:, here] = jnp.broadcast_to(jnp.sum(q * q, 0, keepdims=True), (8, lanes))
        fill(terms, i * lanes, -2.0 * q, RIGHT, 0)


def take_keys(refs, lanes, stack):
    for i, ref in enumerate(refs):
        fill(stack, i * lanes, ref[:lanes, :], LEFT, 1)


def scan(
    inverse_ref, refs, stack, terms, low, totals, *, first, columns, subs, rows, rounds
):
    lanes = subs * rows
    count = terms.shape[1]
    part = lax.dot_general(stack[...], terms[...], NN, preferred_element_type=jnp.float32)
    inverse = [wide(LOG2E * inverse_ref[t : t + 1, :], count) for t in range(rounds)]
    for i, ref in enumerate(refs):
        keys = ref[:lanes, :]
        norm = jnp.sum(keys * keys, -1, keepdims=True)
        for sub in range(subs):
            mine = slice(sub * rows, (sub + 1) * rows)
            tile = part[i * lanes + sub * rows : i * lanes + (sub + 1) * rows] + norm[mine]
            smallest = jnp.min(tile, 0, keepdims=True)
            gap = smallest - tile
            at = (first + i) * subs + sub
            low[at : at + 1, columns] = smallest
            for turn in range(rounds):
                totals[turn, at : at + 1, columns] = jnp.sum(
                    jnp.exp2(gap * inverse[turn]), 0, keepdims=True
                )


def early_kernel(inverse_ref, *refs, near, chunks, subs, rows, rounds):
    lanes = subs * rows
    key_refs = refs[:near]
    query_refs = refs[near : near + chunks]
    terms, norm, stack, low, totals = refs[near + chunks :]
    take_queries(query_refs, lanes, terms, norm)
    take_keys(key_refs, lanes, stack)
    scan(
        inverse_ref,
        key_refs,
        stack,
        terms,
        low,
        totals,
        first=0,
        columns=slice(None),
        subs=subs,
        rows=rows,
        rounds=rounds,
    )


def middle_kernel(
    inverse_ref, stack, low_ref, totals_ref, *refs, near, chunks, subs, rows, rounds
):
    lanes = subs * rows
    key_refs = refs[:near]
    query_refs = refs[near : near + chunks]
    terms, norm, low, totals = refs[near + chunks :]
    before = low_ref.shape[1]
    count = low.shape[1]
    low[:, :before] = low_ref[...]
    totals[:, :, :before] = totals_ref[...]
    take_queries(query_refs, lanes, terms, norm)
    scan(
        inverse_ref,
        key_refs,
        stack,
        terms,
        low,
        totals,
        first=0,
        columns=slice(before, count),
        subs=subs,
        rows=rows,
        rounds=rounds,
    )


def score_kernel(
    inverse_ref,
    hot_ref,
    picked_ref,
    near_terms,
    near_norm,
    far_terms,
    far_norm,
    near_low,
    near_totals,
    *refs,
    chunks,
    later,
    near,
    groups,
    subs,
    rows,
    rounds,
    pairs,
    members,
):
    out_ref, stack, low, totals = refs[-4:]
    key_refs = refs[:-4]
    lanes = subs * rows
    width = key_refs[0].shape[1]
    before = len(chunks) * lanes
    count = before + len(later) * lanes
    cross_at, norm_at, centre_at, _ = layout(groups, rounds, pairs, width, lanes)
    take_keys(key_refs, lanes, stack)
    for terms, columns in ((near_terms, slice(0, before)), (far_terms, slice(before, count))):
        scan(
            inverse_ref,
            key_refs,
            stack,
            terms,
            low,
            totals,
            first=near,
            columns=columns,
            subs=subs,
            rows=rows,
            rounds=rounds,
        )
    done = near * subs
    low[:done, :] = near_low[...]
    totals[:, :done, :] = near_totals[...]
    centre = picked_ref[...] / members
    a = split(centre)
    left = jnp.concatenate([a[k] for k in LEFT], 1)
    cross = jnp.concatenate(
        [
            lax.dot_general(left, right[...], NN, preferred_element_type=jnp.float32)
            for right in (near_terms, far_terms)
        ],
        1,
    )
    query_norm = jnp.concatenate([near_norm[:1, :], far_norm[:1, :]], 1)
    nearest = low[...] + query_norm
    hot = hot_ref[...]
    lane = lax.broadcasted_iota(jnp.int32, (pairs, lanes), 1) // rows
    every = tuple(chunks) + tuple(later)
    for turn in range(rounds):
        value = jnp.log(totals[turn]) - nearest * wide(inverse_ref[turn : turn + 1, :], count)
        chosen = lax.dot_general(
            hot, value, NN, precision=HIGH, preferred_element_type=jnp.float32
        )
        for i, k in enumerate(every):
            piece = chosen[:, i * lanes : (i + 1) * lanes]
            merged = piece[:pairs]
            for sub in range(1, subs):
                merged = jnp.where(lane == sub, piece[sub * pairs : (sub + 1) * pairs], merged)
            at = (k * rounds + turn) * pairs
            out_ref[at : at + pairs, :] = merged
    for i, k in enumerate(every):
        out_ref[cross_at + k * rounds : cross_at + (k + 1) * rounds, :] = cross[
            :rounds, i * lanes : (i + 1) * lanes
        ]
        out_ref[norm_at + k : norm_at + k + 1, :] = query_norm[:, i * lanes : (i + 1) * lanes]
    for turn in range(rounds):
        for c in range(width // lanes):
            at = centre_at + turn * (width // lanes) + c
            out_ref[at : at + 1, :] = centre[turn : turn + 1, c * lanes : (c + 1) * lanes]


def finish_kernel(inverse_ref, *refs, groups, subs, rows, rounds, pairs, width):
    parts = refs[:groups]
    out_ref = refs[groups]
    lanes = subs * rows
    cross_at, norm_at, centre_at, _ = layout(groups, rounds, pairs, width, lanes)
    step = rounds * pairs
    sums = []
    cross = []
    for k in range(groups):
        pieces = [parts[j][(k ^ j) * step : ((k ^ j) + 1) * step, :] for j in range(groups)]
        peak = functools.reduce(jnp.maximum, pieces)
        total = sum(jnp.exp(piece - peak) for piece in pieces)
        sums.append(peak + jnp.log(total))
        at = [cross_at + (k ^ j) * rounds for j in range(groups)]
        cross.append(sum(parts[j][at[j] : at[j] + rounds, :] for j in range(groups)))
    kernel = jnp.concatenate(sums, 0).reshape(groups * rounds, pairs, lanes)
    weighted = jnp.sum(kernel, 1) / pairs
    cross = jnp.concatenate(cross, 0)
    halves = width // lanes
    centre = sum(part[centre_at : centre_at + rounds * halves, :] for part in parts)
    centre_sq = jnp.sum(centre * centre, -1, keepdims=True)
    group_of = lax.broadcasted_iota(jnp.int32, (1, lanes), 1) // rows
    line = lax.broadcasted_iota(jnp.int32, (groups * rounds, lanes), 0)
    inverse = jnp.zeros((groups * rounds, lanes), jnp.float32)
    constant = jnp.zeros((groups * rounds, lanes), jnp.float32)
    norm = jnp.zeros((groups * rounds, lanes), jnp.float32)
    for turn in range(rounds):
        mine = line % rounds == turn
        inverse = jnp.where(mine, inverse_ref[turn : turn + 1, :], inverse)
        square = sum(
            centre_sq[turn * halves + c : turn * halves + c + 1, :] for c in range(halves)
        )
        constant = jnp.where(mine, square, constant)
    for k in range(groups):
        norm = jnp.where(line // rounds == k, parts[0][norm_at + k : norm_at + k + 1, :], norm)
    logits = weighted - (norm + cross + constant) * inverse

    def over_draws(value, combine, reduce, neutral):
        shift = rounds
        while shift < groups * rounds:
            value = combine(value, pltpu.roll(value, shift, 0))
            shift *= 2
        result = value
        for sub in range(subs):
            here = reduce(jnp.where(group_of == sub, value, neutral), -1, keepdims=True)
            result = jnp.where(group_of == sub, here, result)
        return result

    peak = over_draws(logits, jnp.maximum, jnp.max, -jnp.inf)
    shifted = logits - peak
    total = over_draws(jnp.exp(shifted), jnp.add, jnp.sum, 0.0)
    value = shifted - jnp.log(total)
    for turn in range(rounds):
        for sub in range(subs):
            out_ref[turn, sub : sub + 1, :] = value[
                turn : turn + 1, sub * rows : (sub + 1) * rows
            ]


def program(samples, pair_table, assignment, band_index):
    subs, rows, width = samples.shape
    rounds = assignment.shape[0]
    pairs = pair_table.shape[1]
    groups = lax.axis_size("grp")
    blocks = lax.axis_size("blk")
    members = subs * blocks
    lanes = subs * rows

    def over(axis, size, value, k):
        return lax.ppermute(value, axis, [(i, i ^ k) for i in range(size)])

    vmem = pl.BlockSpec(memory_space=pltpu.VMEM)
    hbm = pl.BlockSpec(memory_space=pltpu.HBM)

    def call(kernel, shapes, arrays, scratch=(), **sizes):
        one = not isinstance(shapes, list)
        outs = [
            jax.ShapeDtypeStruct(shape[:-1], shape[-1])
            for shape in ([shapes] if one else shapes)
        ]
        return pl.pallas_call(
            functools.partial(kernel, **sizes),
            out_shape=outs[0] if one else outs,
            in_specs=[vmem] * len(arrays),
            out_specs=vmem if one else [vmem] * len(outs),
            scratch_shapes=[pltpu.VMEM(shape[:-1], shape[-1]) for shape in scratch],
            compiler_params=pltpu.CompilerParams(
                vmem_limit_bytes=(16 if blocks <= 8 else 48) * 2**20
            ),
        )(*arrays)

    f32, bf16 = jnp.float32, jnp.bfloat16
    x = samples.reshape(lanes, width)
    queries = {k: over("grp", groups, x, k) for k in range(groups - 1, 0, -1)}
    own, hot, inverse = pl.pallas_call(
        functools.partial(prepare_kernel, subs=subs, rows=rows, rounds=rounds, pairs=pairs),
        out_shape=[
            jax.ShapeDtypeStruct((lanes + 8, width), f32),
            jax.ShapeDtypeStruct((subs * pairs, members), f32),
            jax.ShapeDtypeStruct((rounds, lanes), f32),
        ],
        in_specs=[hbm] * 4,
        out_specs=[vmem] * 3,
        scratch_shapes=[
            pltpu.SMEM((rounds, subs), jnp.int32),
            pltpu.SMEM((subs, pairs), jnp.int32),
            pltpu.SMEM((rounds,), jnp.int32),
            pltpu.SemaphoreType.DMA((4,)),
        ],
        compiler_params=pltpu.CompilerParams(vmem_limit_bytes=4 * 2**20),
        name="prepare",
    )(
        *[
            pltpu.with_memory_space_constraint(value, pltpu.HBM)
            for value in (assignment, pair_table, band_index, x)
        ]
    )
    keys = {0: own}
    for k in range(2, blocks, 2):
        keys[k] = over("blk", blocks, own if k > 2 else x, k)
    for k in range(0, blocks, 2):
        sent = keys[k] if k else x
        keys[k ^ 1] = over("blk", blocks, sent, 1)
    picked = own[lanes:]
    others = [over("blk", blocks, picked, k) for k in range(2, 4, 2)]
    picked = sum(others, picked)
    picked = picked + over("blk", blocks, picked, 1)
    picked = sum([keys[k][lanes:] for k in range(4, blocks)], picked)
    queries[0] = own
    height = layout(groups, rounds, pairs, width, lanes)[-1]
    order = CHUNKS if groups == len(CHUNKS) else tuple(range(groups))
    chunks, later = order[: groups // 2], order[groups // 2 :]
    near = blocks // 2
    before, after = len(chunks) * lanes, len(later) * lanes
    sizes = {"subs": subs, "rows": rows, "rounds": rounds}
    near_terms, near_norm, stack, low, totals = call(
        early_kernel,
        [
            (len(RIGHT) * width, before, bf16),
            (8, before, f32),
            (near * lanes, len(LEFT) * width, bf16),
            (near * subs, before, f32),
            (rounds, near * subs, before, f32),
        ],
        [inverse] + [keys[k] for k in range(near)] + [queries[k] for k in chunks],
        near=near,
        chunks=len(chunks),
        **sizes,
    )
    far_terms, far_norm, low, totals = call(
        middle_kernel,
        [
            (len(RIGHT) * width, after, bf16),
            (8, after, f32),
            (near * subs, before + after, f32),
            (rounds, near * subs, before + after, f32),
        ],
        [inverse, stack, low, totals]
        + [keys[k] for k in range(near)]
        + [queries[k] for k in later],
        near=near,
        chunks=len(later),
        **sizes,
    )
    part = call(
        score_kernel,
        (height, lanes, f32),
        [inverse, hot, picked, near_terms, near_norm, far_terms, far_norm, low, totals]
        + [keys[k] for k in range(near, blocks)],
        scratch=[
            ((blocks - near) * lanes, len(LEFT) * width, bf16),
            (members, before + after, f32),
            (rounds, members, before + after, f32),
        ],
        chunks=chunks,
        later=later,
        near=near,
        groups=groups,
        pairs=pairs,
        members=members,
        **sizes,
    )
    parts = {k: over("grp", groups, part, k) for k in range(groups - 1, 0, -1)}
    parts[0] = part
    return call(
        finish_kernel,
        (rounds, subs, rows, f32),
        [inverse] + [parts[k] for k in range(groups)],
        groups=groups,
        pairs=pairs,
        width=width,
        **sizes,
    )


CHUNKS = (0, 2, 3, 1)


def solution(mesh):
    return jax.shard_map(
        program,
        mesh=mesh,
        in_specs=(P("blk", "grp", None), P("blk", None), P(None, "blk"), P()),
        out_specs=P(None, "blk", "grp"),
        check_vma=False,
    )
```

```python
import functools

import jax
import jax.numpy as jnp
from jax import lax
from jax.experimental import pallas as pl
from jax.experimental.pallas import tpu as pltpu
from jax.sharding import PartitionSpec as P


HIGH = lax.Precision.HIGHEST
NN = (((1,), (0,)), ((), ()))
LOG2E = 1.4426950408889634
LEFT = (0, 0, 1, 1, 0, 2)
RIGHT = (0, 1, 0, 1, 2, 0)


def split(value):
    first = value.astype(jnp.bfloat16)
    rest = value - first.astype(jnp.float32)
    second = rest.astype(jnp.bfloat16)
    third = (rest - second.astype(jnp.float32)).astype(jnp.bfloat16)
    return first, second, third


def fill(stack, at, value, order, axis):
    parts = split(value)
    for i, k in enumerate(order):
        size = value.shape[axis]
        if axis:
            stack[at : at + value.shape[0], i * size : (i + 1) * size] = parts[k]
        else:
            stack[i * size : (i + 1) * size, at : at + value.shape[1]] = parts[k]


def prepare_kernel(
    assign_hbm,
    table_hbm,
    band_hbm,
    x_hbm,
    out_ref,
    hot_ref,
    inverse_ref,
    assign_ref,
    table_ref,
    band_ref,
    sems,
    *,
    subs,
    rows,
    rounds,
    pairs,
):
    lanes = subs * rows
    width = out_ref.shape[1]
    copies = [
        pltpu.make_async_copy(source, target, sems.at[i])
        for i, (source, target) in enumerate(
            (
                (assign_hbm, assign_ref),
                (band_hbm, band_ref),
                (table_hbm, table_ref),
                (x_hbm, out_ref.at[pl.ds(0, lanes)]),
            )
        )
    ]
    for copy in copies:
        copy.start()
    for copy in copies[:-1]:
        copy.wait()
    block, first = lax.axis_index("blk"), lax.axis_index("grp") * rows
    lane = lax.broadcasted_iota(jnp.int32, (8, lanes), 1)
    line = lax.broadcasted_iota(jnp.int32, (8, lanes), 0)
    weight = jnp.zeros((8, lanes), jnp.float32)
    for turn in range(rounds):
        for sub in range(subs):
            local = assign_ref[turn, sub] - first
            inside = jnp.logical_and(local >= 0, local < rows)
            target = jnp.where(inside, sub * rows + local, -1)
            weight = jnp.where((line == turn) & (lane == target), 1.0, weight)
        index = jnp.full((1, lanes), band_ref[turn], jnp.int32).astype(jnp.float32)
        band_sq = width * (1.0 + index / 256.0) / 32.0
        inverse_ref[turn : turn + 1, :] = 1.0 / (2.0 * band_sq)
    members = hot_ref.shape[1]
    column = lax.broadcasted_iota(jnp.int32, (8, members), 1)
    line = lax.broadcasted_iota(jnp.int32, (8, members), 0)
    for base in range(0, subs * pairs, 8):
        target = jnp.zeros((8, members), jnp.int32)
        for i in range(8):
            entry = table_ref[(base + i) // pairs, (base + i) % pairs]
            owner = lax.div(entry, jnp.int32(subs))
            at = (owner ^ block) * subs + (entry - owner * subs)
            target = jnp.where(line == i, at, target)
        hot_ref[base : base + 8, :] = (column == target).astype(jnp.float32)
    copies[-1].wait()
    out_ref[lanes:, :] = lax.dot_general(
        weight, out_ref[:lanes, :], NN, precision=HIGH, preferred_element_type=jnp.float32
    )


def layout(groups, rounds, pairs, width, lanes):
    cross = groups * rounds * pairs
    norm = cross + groups * rounds
    centre = norm + groups
    height = centre + rounds * (width // lanes)
    return cross, norm, centre, -(-height // 8) * 8


def wide(row, count):
    return jnp.concatenate([row] * (count // row.shape[1]), 1)


def take_queries(refs, lanes, terms, norm):
    for i, ref in enumerate(refs):
        q = ref[:lanes, :].T
        here = slice(i * lanes, (i + 1) * lanes)
        norm[:, here] = jnp.broadcast_to(jnp.sum(q * q, 0, keepdims=True), (8, lanes))
        fill(terms, i * lanes, -2.0 * q, RIGHT, 0)


def take_keys(refs, lanes, stack):
    for i, ref in enumerate(refs):
        fill(stack, i * lanes, ref[:lanes, :], LEFT, 1)


def scan(
    inverse_ref, refs, stack, terms, low, totals, *, first, columns, subs, rows, rounds
):
    lanes = subs * rows
    count = terms.shape[1]
    part = lax.dot_general(stack[...], terms[...], NN, preferred_element_type=jnp.float32)
    inverse = [wide(LOG2E * inverse_ref[t : t + 1, :], count) for t in range(rounds)]
    for i, ref in enumerate(refs):
        keys = ref[:lanes, :]
        norm = jnp.sum(keys * keys, -1, keepdims=True)
        for sub in range(subs):
            mine = slice(sub * rows, (sub + 1) * rows)
            tile = part[i * lanes + sub * rows : i * lanes + (sub + 1) * rows] + norm[mine]
            smallest = jnp.min(tile, 0, keepdims=True)
            gap = smallest - tile
            at = (first + i) * subs + sub
            low[at : at + 1, columns] = smallest
            for turn in range(rounds):
                totals[turn, at : at + 1, columns] = jnp.sum(
                    jnp.exp2(gap * inverse[turn]), 0, keepdims=True
                )


def early_kernel(inverse_ref, *refs, near, chunks, subs, rows, rounds):
    lanes = subs * rows
    key_refs = refs[:near]
    query_refs = refs[near : near + chunks]
    terms, norm, stack, low, totals = refs[near + chunks :]
    take_queries(query_refs, lanes, terms, norm)
    take_keys(key_refs, lanes, stack)
    scan(
        inverse_ref,
        key_refs,
        stack,
        terms,
        low,
        totals,
        first=0,
        columns=slice(None),
        subs=subs,
        rows=rows,
        rounds=rounds,
    )


def middle_kernel(
    inverse_ref, stack, low_ref, totals_ref, *refs, near, chunks, subs, rows, rounds
):
    lanes = subs * rows
    key_refs = refs[:near]
    query_refs = refs[near : near + chunks]
    terms, norm, low, totals = refs[near + chunks :]
    before = low_ref.shape[1]
    count = low.shape[1]
    low[:, :before] = low_ref[...]
    totals[:, :, :before] = totals_ref[...]
    take_queries(query_refs, lanes, terms, norm)
    scan(
        inverse_ref,
        key_refs,
        stack,
        terms,
        low,
        totals,
        first=0,
        columns=slice(before, count),
        subs=subs,
        rows=rows,
        rounds=rounds,
    )


def score_kernel(
    inverse_ref,
    hot_ref,
    picked_ref,
    near_terms,
    near_norm,
    far_terms,
    far_norm,
    near_low,
    near_totals,
    *refs,
    chunks,
    later,
    near,
    groups,
    subs,
    rows,
    rounds,
    pairs,
    members,
):
    out_ref, stack, low, totals = refs[-4:]
    key_refs = refs[:-4]
    lanes = subs * rows
    width = key_refs[0].shape[1]
    before = len(chunks) * lanes
    count = before + len(later) * lanes
    cross_at, norm_at, centre_at, _ = layout(groups, rounds, pairs, width, lanes)
    take_keys(key_refs, lanes, stack)
    for terms, columns in ((near_terms, slice(0, before)), (far_terms, slice(before, count))):
        scan(
            inverse_ref,
            key_refs,
            stack,
            terms,
            low,
            totals,
            first=near,
            columns=columns,
            subs=subs,
            rows=rows,
            rounds=rounds,
        )
    done = near * subs
    low[:done, :] = near_low[...]
    totals[:, :done, :] = near_totals[...]
    centre = picked_ref[...] / members
    a = split(centre)
    left = jnp.concatenate([a[k] for k in LEFT], 1)
    cross = jnp.concatenate(
        [
            lax.dot_general(left, right[...], NN, preferred_element_type=jnp.float32)
            for right in (near_terms, far_terms)
        ],
        1,
    )
    query_norm = jnp.concatenate([near_norm[:1, :], far_norm[:1, :]], 1)
    nearest = low[...] + query_norm
    hot = hot_ref[...]
    lane = lax.broadcasted_iota(jnp.int32, (pairs, lanes), 1) // rows
    every = tuple(chunks) + tuple(later)
    for turn in range(rounds):
        value = jnp.log(totals[turn]) - nearest * wide(inverse_ref[turn : turn + 1, :], count)
        chosen = lax.dot_general(
            hot, value, NN, precision=HIGH, preferred_element_type=jnp.float32
        )
        for i, k in enumerate(every):
            piece = chosen[:, i * lanes : (i + 1) * lanes]
            merged = piece[:pairs]
            for sub in range(1, subs):
                merged = jnp.where(lane == sub, piece[sub * pairs : (sub + 1) * pairs], merged)
            at = (k * rounds + turn) * pairs
            out_ref[at : at + pairs, :] = merged
    for i, k in enumerate(every):
        out_ref[cross_at + k * rounds : cross_at + (k + 1) * rounds, :] = cross[
            :rounds, i * lanes : (i + 1) * lanes
        ]
        out_ref[norm_at + k : norm_at + k + 1, :] = query_norm[:, i * lanes : (i + 1) * lanes]
    for turn in range(rounds):
        for c in range(width // lanes):
            at = centre_at + turn * (width // lanes) + c
            out_ref[at : at + 1, :] = centre[turn : turn + 1, c * lanes : (c + 1) * lanes]


def finish_kernel(inverse_ref, *refs, groups, subs, rows, rounds, pairs, width):
    parts = refs[:groups]
    out_ref = refs[groups]
    lanes = subs * rows
    cross_at, norm_at, centre_at, _ = layout(groups, rounds, pairs, width, lanes)
    step = rounds * pairs
    sums = []
    cross = []
    for k in range(groups):
        pieces = [parts[j][(k ^ j) * step : ((k ^ j) + 1) * step, :] for j in range(groups)]
        peak = functools.reduce(jnp.maximum, pieces)
        total = sum(jnp.exp(piece - peak) for piece in pieces)
        sums.append(peak + jnp.log(total))
        at = [cross_at + (k ^ j) * rounds for j in range(groups)]
        cross.append(sum(parts[j][at[j] : at[j] + rounds, :] for j in range(groups)))
    kernel = jnp.concatenate(sums, 0).reshape(groups * rounds, pairs, lanes)
    weighted = jnp.sum(kernel, 1) / pairs
    cross = jnp.concatenate(cross, 0)
    halves = width // lanes
    centre = sum(part[centre_at : centre_at + rounds * halves, :] for part in parts)
    centre_sq = jnp.sum(centre * centre, -1, keepdims=True)
    group_of = lax.broadcasted_iota(jnp.int32, (1, lanes), 1) // rows
    line = lax.broadcasted_iota(jnp.int32, (groups * rounds, lanes), 0)
    inverse = jnp.zeros((groups * rounds, lanes), jnp.float32)
    constant = jnp.zeros((groups * rounds, lanes), jnp.float32)
    norm = jnp.zeros((groups * rounds, lanes), jnp.float32)
    for turn in range(rounds):
        mine = line % rounds == turn
        inverse = jnp.where(mine, inverse_ref[turn : turn + 1, :], inverse)
        square = sum(
            centre_sq[turn * halves + c : turn * halves + c + 1, :] for c in range(halves)
        )
        constant = jnp.where(mine, square, constant)
    for k in range(groups):
        norm = jnp.where(line // rounds == k, parts[0][norm_at + k : norm_at + k + 1, :], norm)
    logits = weighted - (norm + cross + constant) * inverse

    def over_draws(value, combine, reduce, neutral):
        shift = rounds
        while shift < groups * rounds:
            value = combine(value, pltpu.roll(value, shift, 0))
            shift *= 2
        result = value
        for sub in range(subs):
            here = reduce(jnp.where(group_of == sub, value, neutral), -1, keepdims=True)
            result = jnp.where(group_of == sub, here, result)
        return result

    peak = over_draws(logits, jnp.maximum, jnp.max, -jnp.inf)
    shifted = logits - peak
    total = over_draws(jnp.exp(shifted), jnp.add, jnp.sum, 0.0)
    value = shifted - jnp.log(total)
    for turn in range(rounds):
        for sub in range(subs):
            out_ref[turn, sub : sub + 1, :] = value[
                turn : turn + 1, sub * rows : (sub + 1) * rows
            ]


def program(samples, pair_table, assignment, band_index):
    subs, rows, width = samples.shape
    rounds = assignment.shape[0]
    pairs = pair_table.shape[1]
    groups = lax.axis_size("grp")
    blocks = lax.axis_size("blk")
    members = subs * blocks
    lanes = subs * rows

    def over(axis, size, value, k):
        return lax.ppermute(value, axis, [(i, i ^ k) for i in range(size)])

    vmem = pl.BlockSpec(memory_space=pltpu.VMEM)
    hbm = pl.BlockSpec(memory_space=pltpu.HBM)

    def call(kernel, shapes, arrays, scratch=(), **sizes):
        one = not isinstance(shapes, list)
        outs = [
            jax.ShapeDtypeStruct(shape[:-1], shape[-1])
            for shape in ([shapes] if one else shapes)
        ]
        return pl.pallas_call(
            functools.partial(kernel, **sizes),
            out_shape=outs[0] if one else outs,
            in_specs=[vmem] * len(arrays),
            out_specs=vmem if one else [vmem] * len(outs),
            scratch_shapes=[pltpu.VMEM(shape[:-1], shape[-1]) for shape in scratch],
            compiler_params=pltpu.CompilerParams(
                vmem_limit_bytes=(16 if blocks <= 8 else 48) * 2**20
            ),
        )(*arrays)

    f32, bf16 = jnp.float32, jnp.bfloat16
    x = samples.reshape(lanes, width)
    queries = {k: over("grp", groups, x, k) for k in range(groups - 1, 0, -1)}
    own, hot, inverse = pl.pallas_call(
        functools.partial(prepare_kernel, subs=subs, rows=rows, rounds=rounds, pairs=pairs),
        out_shape=[
            jax.ShapeDtypeStruct((lanes + 8, width), f32),
            jax.ShapeDtypeStruct((subs * pairs, members), f32),
            jax.ShapeDtypeStruct((rounds, lanes), f32),
        ],
        in_specs=[hbm] * 4,
        out_specs=[vmem] * 3,
        scratch_shapes=[
            pltpu.SMEM((rounds, subs), jnp.int32),
            pltpu.SMEM((subs, pairs), jnp.int32),
            pltpu.SMEM((rounds,), jnp.int32),
            pltpu.SemaphoreType.DMA((4,)),
        ],
        compiler_params=pltpu.CompilerParams(vmem_limit_bytes=4 * 2**20),
        name="prepare",
    )(
        *[
            pltpu.with_memory_space_constraint(value, pltpu.HBM)
            for value in (assignment, pair_table, band_index, x)
        ]
    )
    keys = {0: own}
    for k in range(2, blocks, 2):
        keys[k] = over("blk", blocks, own, k)
    for k in range(0, blocks, 2):
        keys[k ^ 1] = over("blk", blocks, keys[k], 1)
    picked = sum([keys[k][lanes:] for k in range(1, blocks)], own[lanes:])
    queries[0] = own
    height = layout(groups, rounds, pairs, width, lanes)[-1]
    order = CHUNKS if groups == len(CHUNKS) else tuple(range(groups))
    chunks, later = order[: groups // 2], order[groups // 2 :]
    near = blocks // 2
    before, after = len(chunks) * lanes, len(later) * lanes
    sizes = {"subs": subs, "rows": rows, "rounds": rounds}
    near_terms, near_norm, stack, low, totals = call(
        early_kernel,
        [
            (len(RIGHT) * width, before, bf16),
            (8, before, f32),
            (near * lanes, len(LEFT) * width, bf16),
            (near * subs, before, f32),
            (rounds, near * subs, before, f32),
        ],
        [inverse] + [keys[k] for k in range(near)] + [queries[k] for k in chunks],
        near=near,
        chunks=len(chunks),
        **sizes,
    )
    far_terms, far_norm, low, totals = call(
        middle_kernel,
        [
            (len(RIGHT) * width, after, bf16),
            (8, after, f32),
            (near * subs, before + after, f32),
            (rounds, near * subs, before + after, f32),
        ],
        [inverse, stack, low, totals]
        + [keys[k] for k in range(near)]
        + [queries[k] for k in later],
        near=near,
        chunks=len(later),
        **sizes,
    )
    part = call(
        score_kernel,
        (height, lanes, f32),
        [inverse, hot, picked, near_terms, near_norm, far_terms, far_norm, low, totals]
        + [keys[k] for k in range(near, blocks)],
        scratch=[
            ((blocks - near) * lanes, len(LEFT) * width, bf16),
            (members, before + after, f32),
            (rounds, members, before + after, f32),
        ],
        chunks=chunks,
        later=later,
        near=near,
        groups=groups,
        pairs=pairs,
        members=members,
        **sizes,
    )
    parts = {k: over("grp", groups, part, k) for k in range(groups - 1, 0, -1)}
    parts[0] = part
    return call(
        finish_kernel,
        (rounds, subs, rows, f32),
        [inverse] + [parts[k] for k in range(groups)],
        groups=groups,
        pairs=pairs,
        width=width,
        **sizes,
    )


CHUNKS = (0, 3, 2, 1)


def solution(mesh):
    return jax.shard_map(
        program,
        mesh=mesh,
        in_specs=(P("blk", "grp", None), P("blk", None), P(None, "blk"), P()),
        out_specs=P(None, "blk", "grp"),
        check_vma=False,
    )
```
